32 devices in a mesh: row: 8 (over z, x), col: 4 (over y, core).
Axes of the slice: x: 2, y: 2, z: 4, core: 2. Of those that a mesh axis runs over, the one named last changes fastest.
Arguments:
- grad: bfloat16 [16384, 1024], P(('row', 'col')), may hold values from -2500 to 2500
- left_root: bfloat16 [16384, 1024], P(('row', 'col')), may hold values from -0.051 to 3, as said below
- right_root: bfloat16 [16384, 1024], P(('row', 'col')), may hold values from -0.051 to 3, as said below
Outputs:
- update: bfloat16 [16384, 1024], P(('row', 'col'))
The draws below stay inside these ranges and needn't reach their ends.
Inputs may be any that keep to these rules, and one draw needn't show every extreme that they name: `left_root`: each block L_b is symmetric and positive definite. `right_root`: each block R_b is symmetric and positive definite.
All inputs are finite; a program needn't handle non-finite values.
Results may differ from the reference program's by a relative error of at most 0.0049.
Values may be sent and summed in bfloat16 or wider, within the bound.
A program may use at most 64 MiB of HBM per device.

```python
import math
import jax
import jax.numpy as jnp
from jax import lax

BLK = 1024
NB = 16


def root_blocks(key, stream):
    folded = jax.random.fold_in(key, stream)
    k_diagonal, k_entries = jax.random.split(folded)
    diagonal = jnp.exp(jax.random.uniform(k_diagonal, (NB, BLK), jnp.float32, math.log(0.6), math.log(2.0)))
    entries = jnp.clip(jax.random.normal(k_entries, (NB, BLK, BLK), jnp.float32), -4.0, 4.0)
    spread = 0.26
    symmetric = (entries + jnp.swapaxes(entries, 1, 2)) * (spread / math.sqrt(2.0 * BLK))
    symmetric = jnp.clip(symmetric, -0.05, 0.05)
    identity = jnp.eye(BLK, dtype=jnp.float32)
    blocks = symmetric * (1.0 - identity) + diagonal[:, :, None] * identity
    return blocks.reshape(NB * BLK, BLK).astype(jnp.bfloat16)


def draw_left_root(key, part):
    return root_blocks(key, 11)


def draw_right_root(key, part):
    return root_blocks(key, 23)


def draw_grad(key, part):
    k_noise, k_rows, k_cols = jax.random.split(jax.random.fold_in(key, 5), 3)
    position = jnp.arange(NB, dtype=jnp.float32) / max(NB - 1, 1)
    gaussian = jnp.clip(jax.random.normal(k_noise, (NB, BLK, BLK), jnp.float32), -6.0, 6.0)
    row_scale = jnp.exp(jax.random.uniform(k_rows, (NB, BLK), jnp.float32, 0.0, math.log(10.0)))
    col_scale = jnp.exp(jax.random.uniform(k_cols, (NB, BLK), jnp.float32, 0.0, math.log(10.0)))
    block_scale = jnp.sqrt(1.0 + 2.0 * position)
    values = gaussian * row_scale[:, :, None] * col_scale[:, None, :] * block_scale[:, None, None]
    return values.reshape(NB * BLK, BLK).astype(jnp.bfloat16)


def setup_inputs(seed: int = 0) -> dict:
    key_list = jax.random.split(jax.random.key(seed), 4)
    return {
        "grad": draw_grad(jax.random.fold_in(key_list[3], 71), 0),
        "left_root": draw_left_root(jax.random.fold_in(key_list[3], 71), 0),
        "right_root": draw_right_root(jax.random.fold_in(key_list[3], 71), 0),
    }


epsilon = 1e-06
clip_rms = 1.0

def reference(grad, left_root, right_root):
    grad_blocks = grad.reshape(NB, BLK, BLK)
    left_blocks = left_root.reshape(NB, BLK, BLK)
    right_blocks = right_root.reshape(NB, BLK, BLK)
    global_sq = jnp.sum(jnp.square(grad.astype(jnp.float32)))
    entries_all = NB * BLK * BLK
    clip_factor = clip_rms / jnp.sqrt(global_sq / entries_all + epsilon)

    def one_block(operands):
        gradient, left_block, right_block = operands
        product = jnp.dot(gradient, right_block, preferred_element_type=jnp.float32).astype(jnp.bfloat16)
        precond = jnp.dot(left_block, product, preferred_element_type=jnp.float32)
        grad_sq = jnp.sum(jnp.square(gradient.astype(jnp.float32)))
        cond_sq = jnp.sum(precond * precond)
        graft_ratio = jnp.sqrt((grad_sq / (BLK * BLK) + epsilon) / (cond_sq / (BLK * BLK) + epsilon))
        return (clip_factor * graft_ratio * precond).astype(jnp.bfloat16)
    update = lax.map(one_block, (grad_blocks, left_blocks, right_blocks))
    return update.reshape(NB * BLK, BLK)
```

```python
import functools

import jax
import jax.numpy as jnp
from jax import lax
from jax.experimental import pallas as pl
from jax.experimental.pallas import tpu as pltpu
from jax.sharding import PartitionSpec as P

epsilon = 1e-06
clip_rms = 1.0
MESH = pl.DeviceIdType.MESH
F32 = jnp.float32


def nn(a, b):
    return jnp.dot(a, b, preferred_element_type=F32)


def nt(a, b):
    return lax.dot_general(a, b, (((1,), (1,)), ((), ())), preferred_element_type=F32)


def row_sq(x):
    s = jnp.sum(x * x, axis=0, keepdims=True)
    total = s[:, :128]
    for i in range(128, s.shape[1], 128):
        total = total + s[:, i : i + 128]
    return total


def near_far(nr, nc):
    low = 2 if nr % 2 == 0 else 1
    near = [(x, c, b) for x in range(low) for c in range(nc // 2) for b in range(2)]
    far = list(range(nr // low))
    return low, near[1:], far[1:]


def kernel(nr, nc, g_hbm, l_hbm, r_hbm, p_ref, factor_ref,
           ga, gb, ra_own, ra_off, la, lb, rx, ra0, ra1, xa, xb, part,
           near_buf, far_buf, cond_buf, load_sem, send_sem, recv_sem):
    rows = g_hbm.shape[0]
    width = g_hbm.shape[1]
    row, col = lax.axis_index("row"), lax.axis_index("col")
    parity = lax.rem(col, 2)
    low, near, far = near_far(nr, nc)
    x_me, z_me, c_me = lax.rem(row, low), row // low, col // 2

    def near_id(k):
        x, c, b = k
        prow = z_me * low + lax.rem(x_me + x, low)
        pcol = lax.rem(c_me + c, nc // 2) * 2 + lax.rem(parity + b, 2)
        return (prow, pcol)

    def far_id(k):
        return (lax.rem(z_me + k, nr // low) * low + x_me, col)

    partner = (row, c_me * 2 + 1 - parity)

    barrier = pltpu.get_barrier_semaphore()
    for k in near:
        pl.semaphore_signal(barrier, inc=1, device_id=near_id(k), device_id_type=MESH)
    for k in far:
        pl.semaphore_signal(barrier, inc=1, device_id=far_id(k), device_id_type=MESH)

    own = pl.ds(pl.multiple_of(parity * rows, rows), rows)
    off = pl.ds(pl.multiple_of((1 - parity) * rows, rows), rows)
    loads = []
    for i, (src, where, dst) in enumerate(
        ((g_hbm, own, ga), (g_hbm, off, gb), (r_hbm, own, ra_own), (r_hbm, off, ra_off),
         (l_hbm, own, la), (l_hbm, off, lb))
    ):
        loads.append(pltpu.make_async_copy(src.at[:, where], dst, load_sem.at[i]))
        loads[-1].start()

    sends = []

    def send(src, dst, device):
        i = len(sends)
        copy = pltpu.make_async_remote_copy(
            src_ref=src, dst_ref=dst, send_sem=send_sem.at[i], recv_sem=recv_sem.at[i],
            device_id=device, device_id_type=MESH)
        copy.start()
        sends.append(copy)
        return copy

    loads[0].wait()
    sq = row_sq(ga[...].astype(F32))
    loads[1].wait()
    sq = sq + row_sq(gb[...].astype(F32))
    near_buf[0] = sq
    loads[2].wait()
    loads[3].wait()
    ra0[...] = (nn(ga[...], ra_own[...]) + nt(gb[...], ra_off[...])).astype(jnp.bfloat16)

    pl.semaphore_wait(barrier, len(near) + len(far))
    near_copies = [send(near_buf.at[0], near_buf.at[1 + i], near_id(k)) for i, k in enumerate(near)]
    rx_copy = send(ra_own, rx, partner)
    xb_copy = send(ra0, xb, partner)

    part[...] = nn(ga[...], ra_off[...])
    loads[4].wait()
    p_ref[:, own] = nn(la[...], ra0[...])
    rx_copy.wait_recv()
    ra1[...] = (part[...] + nn(gb[...], rx[...])).astype(jnp.bfloat16)
    xa_copy = send(ra1, xa, partner)
    part[...] = nn(la[...], ra1[...])

    block_row = sq
    near_sum = sq
    for i, (k, copy) in enumerate(zip(near, near_copies)):
        copy.wait_recv()
        near_sum = near_sum + near_buf[1 + i]
        if k == (0, 0, 1):
            block_row = sq + near_buf[1 + i]
    far_buf[0] = near_sum
    far_copies = [send(far_buf.at[0], far_buf.at[1 + i], far_id(k)) for i, k in enumerate(far)]

    loads[5].wait()
    xb_copy.wait_recv()
    p1 = part[...] + nn(lb[...], xb[...])
    p_ref[:, off] = p1
    cond = row_sq(p1)
    xa_copy.wait_recv()
    p0 = p_ref[:, own] + nn(lb[...], xa[...])
    p_ref[:, own] = p0
    cond = cond + row_sq(p0)
    cond_buf[0] = cond
    cond_copy = send(cond_buf.at[0], cond_buf.at[1], partner)

    total = near_sum
    for i, copy in enumerate(far_copies):
        copy.wait_recv()
        total = total + far_buf[1 + i]
    cond_copy.wait_recv()
    cond = cond + cond_buf[1]

    count = width * width
    global_sq = jnp.sum(total, axis=1, keepdims=True)
    grad_sq = jnp.sum(block_row, axis=1, keepdims=True)
    cond_sq = jnp.sum(cond, axis=1, keepdims=True)
    clip = clip_rms / jnp.sqrt(global_sq / (nr * nc * rows * width) + epsilon)
    graft = jnp.sqrt((grad_sq / count + epsilon) / (cond_sq / count + epsilon))
    factor_ref[...] = jnp.broadcast_to(clip * graft, factor_ref.shape)
    for copy in sends:
        copy.wait_send()


def shards(nr, nc, grad, left_root, right_root):
    rows, width = grad.shape
    low, near, far = near_far(nr, nc)
    copies = len(near) + len(far) + 4
    quarter = pltpu.VMEM((rows, width // 2), jnp.bfloat16)
    vmem = pl.BlockSpec(memory_space=pltpu.VMEM)
    preconditioned, factor = pl.pallas_call(
        functools.partial(kernel, nr, nc),
        out_shape=(jax.ShapeDtypeStruct((rows, width), F32), jax.ShapeDtypeStruct((8, 128), F32)),
        in_specs=[pl.BlockSpec(memory_space=pltpu.HBM)] * 3,
        out_specs=(vmem, vmem),
        scratch_shapes=[quarter] * 11
        + [
            pltpu.VMEM((rows, width // 2), F32),
            pltpu.VMEM((1 + len(near), 1, 128), F32),
            pltpu.VMEM((1 + len(far), 1, 128), F32),
            pltpu.VMEM((2, 1, 128), F32),
            pltpu.SemaphoreType.DMA((6,)),
            pltpu.SemaphoreType.DMA((copies,)),
            pltpu.SemaphoreType.DMA((copies,)),
        ],
        compiler_params=pltpu.CompilerParams(
            collective_id=0, has_side_effects=True, vmem_limit_bytes=64_900_000
        ),
        name="shampoo",
    )(grad, left_root, right_root)
    return (factor[0, 0] * preconditioned).astype(jnp.bfloat16)


def solution(mesh):
    placed = (P(("row", "col"), None), P(("row", "col"), None), P(("row", "col"), None))
    return jax.shard_map(
        functools.partial(shards, mesh.shape["row"], mesh.shape["col"]),
        mesh=mesh, in_specs=placed, out_specs=P(("row", "col"), None), check_vma=False
    )
```

```python
import functools

import jax
import jax.numpy as jnp
from jax import lax
from jax.experimental import pallas as pl
from jax.experimental.pallas import tpu as pltpu
from jax.sharding import PartitionSpec as P

epsilon = 1e-06
clip_rms = 1.0
MESH = pl.DeviceIdType.MESH
F32 = jnp.float32


def nn(a, b):
    return jnp.dot(a, b, preferred_element_type=F32)


def nt(a, b):
    return lax.dot_general(a, b, (((1,), (1,)), ((), ())), preferred_element_type=F32)


def row_sq(x):
    s = jnp.sum(x * x, axis=0, keepdims=True)
    total = s[:, :128]
    for i in range(128, s.shape[1], 128):
        total = total + s[:, i : i + 128]
    return total


def near_far(nr, nc):
    low = 2 if nr % 2 == 0 else 1
    near = [(x, c, b) for x in range(low) for c in range(nc // 2) for b in range(2)]
    far = list(range(nr // low))
    return low, near[1:], far[1:]


def kernel(nr, nc, g_hbm, l_hbm, r_hbm, p_ref, factor_ref,
           ga, gb, ra_own, ra_off, la, lb, rx, ra0, ra1, xa, xb, part,
           near_buf, far_buf, cond_buf, load_sem, send_sem, recv_sem):
    rows = g_hbm.shape[0]
    width = g_hbm.shape[1]
    row, col = lax.axis_index("row"), lax.axis_index("col")
    parity = lax.rem(col, 2)
    low, near, far = near_far(nr, nc)
    x_me, z_me, c_me = lax.rem(row, low), row // low, col // 2

    def near_id(k):
        x, c, b = k
        prow = z_me * low + lax.rem(x_me + x, low)
        pcol = lax.rem(c_me + c, nc // 2) * 2 + lax.rem(parity + b, 2)
        return (prow, pcol)

    def far_id(k):
        return (lax.rem(z_me + k, nr // low) * low + x_me, col)

    partner = (row, c_me * 2 + 1 - parity)

    barrier = pltpu.get_barrier_semaphore()
    for k in near:
        pl.semaphore_signal(barrier, inc=1, device_id=near_id(k), device_id_type=MESH)
    for k in far:
        pl.semaphore_signal(barrier, inc=1, device_id=far_id(k), device_id_type=MESH)

    own = pl.ds(pl.multiple_of(parity * rows, rows), rows)
    off = pl.ds(pl.multiple_of((1 - parity) * rows, rows), rows)
    loads = []
    for i, (src, where, dst) in enumerate(
        ((g_hbm, own, ga), (g_hbm, off, gb), (r_hbm, own, ra_own), (r_hbm, off, ra_off),
         (l_hbm, own, la), (l_hbm, off, lb))
    ):
        loads.append(pltpu.make_async_copy(src.at[:, where], dst, load_sem.at[i]))
        loads[-1].start()

    sends = []

    def send(src, dst, device):
        i = len(sends)
        copy = pltpu.make_async_remote_copy(
            src_ref=src, dst_ref=dst, send_sem=send_sem.at[i], recv_sem=recv_sem.at[i],
            device_id=device, device_id_type=MESH)
        copy.start()
        sends.append(copy)
        return copy

    loads[0].wait()
    sq = row_sq(ga[...].astype(F32))
    loads[1].wait()
    sq = sq + row_sq(gb[...].astype(F32))
    near_buf[0] = sq
    loads[2].wait()
    loads[3].wait()
    ra0[...] = (nn(ga[...], ra_own[...]) + nt(gb[...], ra_off[...])).astype(jnp.bfloat16)

    pl.semaphore_wait(barrier, len(near) + len(far))
    near_copies = [send(near_buf.at[0], near_buf.at[1 + i], near_id(k)) for i, k in enumerate(near)]
    rx_copy = send(ra_own, rx, partner)
    xb_copy = send(ra0, xb, partner)

    part[...] = nn(ga[...], ra_off[...])
    loads[4].wait()
    p_ref[:, own] = nn(la[...], ra0[...])
    rx_copy.wait_recv()
    ra1[...] = (part[...] + nn(gb[...], rx[...])).astype(jnp.bfloat16)
    xa_copy = send(ra1, xa, partner)
    part[...] = nn(la[...], ra1[...])

    block_row = sq
    near_sum = sq
    for i, (k, copy) in enumerate(zip(near, near_copies)):
        copy.wait_recv()
        near_sum = near_sum + near_buf[1 + i]
        if k == (0, 0, 1):
            block_row = sq + near_buf[1 + i]
    far_buf[0] = near_sum
    far_copies = [send(far_buf.at[0], far_buf.at[1 + i], far_id(k)) for i, k in enumerate(far)]

    loads[5].wait()
    xb_copy.wait_recv()
    p1 = part[...] + nn(lb[...], xb[...])
    p_ref[:, off] = p1
    cond = row_sq(p1)
    xa_copy.wait_recv()
    p0 = p_ref[:, own] + nn(lb[...], xa[...])
    p_ref[:, own] = p0
    cond = cond + row_sq(p0)
    cond_buf[0] = cond
    cond_copy = send(cond_buf.at[0], cond_buf.at[1], partner)

    total = near_sum
    for i, copy in enumerate(far_copies):
        copy.wait_recv()
        total = total + far_buf[1 + i]
    cond_copy.wait_recv()
    cond = cond + cond_buf[1]

    count = width * width
    global_sq = jnp.sum(total, axis=1, keepdims=True)
    grad_sq = jnp.sum(block_row, axis=1, keepdims=True)
    cond_sq = jnp.sum(cond, axis=1, keepdims=True)
    clip = clip_rms / jnp.sqrt(global_sq / (nr * nc * rows * width) + epsilon)
    graft = jnp.sqrt((grad_sq / count + epsilon) / (cond_sq / count + epsilon))
    factor_ref[...] = jnp.broadcast_to(clip * graft, factor_ref.shape)
    for copy in sends:
        copy.wait_send()


CHUNKS = 4


def scale(p_ref, factor_ref, out_hbm, scaled, sem):
    rows = p_ref.shape[0] // CHUNKS
    factor = factor_ref[0:1, 0:1]
    copies = []
    for i in range(CHUNKS):
        part = pl.ds(i * rows, rows)
        scaled[part, :] = (factor * p_ref[part, :]).astype(jnp.bfloat16)
        copies.append(pltpu.make_async_copy(scaled.at[part, :], out_hbm.at[part, :], sem.at[i]))
        copies[-1].start()
    for copy in copies:
        copy.wait()


def shards(nr, nc, grad, left_root, right_root):
    rows, width = grad.shape
    low, near, far = near_far(nr, nc)
    copies = len(near) + len(far) + 4
    quarter = pltpu.VMEM((rows, width // 2), jnp.bfloat16)
    vmem = pl.BlockSpec(memory_space=pltpu.VMEM)
    grad, left_root, right_root = (
        pltpu.with_memory_space_constraint(a, pltpu.HBM) for a in (grad, left_root, right_root)
    )
    preconditioned, factor = pl.pallas_call(
        functools.partial(kernel, nr, nc),
        out_shape=(pltpu.VMEM((rows, width), F32), pltpu.VMEM((1, 128), F32)),
        in_specs=[pl.BlockSpec(memory_space=pltpu.HBM)] * 3,
        out_specs=(vmem, vmem),
        scratch_shapes=[quarter] * 11
        + [
            pltpu.VMEM((rows, width // 2), F32),
            pltpu.VMEM((1 + len(near), 1, 128), F32),
            pltpu.VMEM((1 + len(far), 1, 128), F32),
            pltpu.VMEM((2, 1, 128), F32),
            pltpu.SemaphoreType.DMA((6,)),
            pltpu.SemaphoreType.DMA((copies,)),
            pltpu.SemaphoreType.DMA((copies,)),
        ],
        compiler_params=pltpu.CompilerParams(
            collective_id=0, has_side_effects=True, vmem_limit_bytes=32 * 1024 * 1024
        ),
        name="shampoo",
    )(grad, left_root, right_root)
    return pl.pallas_call(
        scale,
        out_shape=jax.ShapeDtypeStruct((rows, width), jnp.bfloat16),
        in_specs=[vmem, vmem],
        out_specs=pl.BlockSpec(memory_space=pltpu.HBM),
        scratch_shapes=[pltpu.VMEM((rows, width), jnp.bfloat16), pltpu.SemaphoreType.DMA((CHUNKS,))],
        compiler_params=pltpu.CompilerParams(vmem_limit_bytes=16 * 1024 * 1024),
        name="scale",
    )(preconditioned, factor)


def solution(mesh):
    placed = (P(("row", "col"), None), P(("row", "col"), None), P(("row", "col"), None))
    return jax.shard_map(
        functools.partial(shards, mesh.shape["row"], mesh.shape["col"]),
        mesh=mesh, in_specs=placed, out_specs=P(("row", "col"), None), check_vma=False
    )
```

```python
import functools

import jax
import jax.numpy as jnp
from jax import lax
from jax.experimental import pallas as pl
from jax.experimental.pallas import tpu as pltpu
from jax.sharding import PartitionSpec as P

epsilon = 1e-06
clip_rms = 1.0
MESH = pl.DeviceIdType.MESH
F32 = jnp.float32


def nn(a, b):
    return jnp.dot(a, b, preferred_element_type=F32)


def nt(a, b):
    return lax.dot_general(a, b, (((1,), (1,)), ((), ())), preferred_element_type=F32)


def row_sq(x):
    s = jnp.sum(x * x, axis=0, keepdims=True)
    total = s[:, :128]
    for i in range(128, s.shape[1], 128):
        total = total + s[:, i : i + 128]
    return total


def kernel(nr, nc, g_hbm, l_hbm, r_hbm, p_ref, factor_ref,
           ga, gb, ra_own, ra_off, la, lb, rx, ra0, ra1, xa, xb, part,
           sums, pair, load_sem, send_sem, recv_sem, sums_send, sums_recv, ready):
    rows, width = g_hbm.shape
    devices = nr * nc
    row, col = lax.axis_index("row"), lax.axis_index("col")
    parity = lax.rem(col, 2)
    me = row * nc + col
    partner = (row, col + 1 - 2 * parity)

    def place(rank):
        return (lax.div(rank, nc), lax.rem(rank, nc))

    own = pl.ds(pl.multiple_of(parity * rows, rows), rows)
    off = pl.ds(pl.multiple_of((1 - parity) * rows, rows), rows)
    loads = []
    for i, (src, where, dst) in enumerate(
        ((g_hbm, own, ga), (g_hbm, off, gb), (r_hbm, own, ra_own), (r_hbm, off, ra_off),
         (l_hbm, own, la), (l_hbm, off, lb))
    ):
        loads.append(pltpu.make_async_copy(src.at[:, where], dst, load_sem.at[i]))
        loads[-1].start()

    barrier = pltpu.get_barrier_semaphore()

    def greet(rank, _):
        pl.semaphore_signal(barrier, inc=1, device_id=place(rank), device_id_type=MESH)

    lax.fori_loop(me - parity, me, greet, None)
    lax.fori_loop(me + 1, devices, greet, None)
    pl.semaphore_wait(barrier, me + 1 - parity)

    def say_ready(rank, _):
        pl.semaphore_signal(ready, inc=1, device_id=place(rank), device_id_type=MESH)

    lax.fori_loop(0, me, say_ready, None)

    sends = []

    def send(src, dst, device):
        i = len(sends)
        copy = pltpu.make_async_remote_copy(
            src_ref=src, dst_ref=dst, send_sem=send_sem.at[i], recv_sem=recv_sem.at[i],
            device_id=device, device_id_type=MESH)
        copy.start()
        sends.append(copy)
        return copy

    def send_sum(rank, _):
        pltpu.make_async_remote_copy(
            src_ref=pair.at[0], dst_ref=sums.at[me], send_sem=sums_send, recv_sem=sums_recv,
            device_id=place(rank), device_id_type=MESH).start()

    loads[0].wait()
    sq = row_sq(ga[...].astype(F32))
    loads[1].wait()
    sq = sq + row_sq(gb[...].astype(F32))
    pair[0] = sq
    lax.fori_loop(0, me, send_sum, None)
    loads[2].wait()
    rx_copy = send(ra_own, rx, partner)
    loads[3].wait()
    ra0[...] = (nn(ga[...], ra_own[...]) + nt(gb[...], ra_off[...])).astype(jnp.bfloat16)
    xb_copy = send(ra0, xb, partner)

    part[...] = nn(ga[...], ra_off[...])
    loads[4].wait()
    p_ref[:, own] = nn(la[...], ra0[...])
    rx_copy.wait_recv()
    ra1[...] = (part[...] + nn(gb[...], rx[...])).astype(jnp.bfloat16)
    xa_copy = send(ra1, xa, partner)
    part[...] = nn(la[...], ra1[...])

    loads[5].wait()
    xb_copy.wait_recv()
    p1 = part[...] + nn(lb[...], xb[...])
    p_ref[:, off] = p1
    cond = row_sq(p1)
    xa_copy.wait_recv()
    p0 = p_ref[:, own] + nn(lb[...], xa[...])
    p_ref[:, own] = p0
    cond = cond + row_sq(p0)
    pair[1] = cond
    pair_copy = send(pair.at[pl.ds(0, 2)], pair.at[pl.ds(2, 2)], partner)

    @pl.when(me < devices - 1)
    def _():
        pl.semaphore_wait(ready, devices - 1 - me)
        lax.fori_loop(me + 1, devices, send_sum, None)


    count = width * width
    pair_copy.wait_recv()
    grad_sq = jnp.sum(sq + pair[2], axis=1, keepdims=True)
    cond_sq = jnp.sum(cond + pair[3], axis=1, keepdims=True)
    graft = jnp.sqrt((grad_sq / count + epsilon) / (cond_sq / count + epsilon))
    for copy in sends:
        copy.wait_send()

    sums[me] = sq
    others = pl.ds(0, devices - 1)
    pltpu.make_async_copy(sums.at[others], sums.at[others], sums_recv).wait()
    global_sq = jnp.sum(jnp.sum(sums[...], axis=0), axis=1, keepdims=True)
    clip = clip_rms / jnp.sqrt(global_sq / (devices * rows * width) + epsilon)
    factor_ref[...] = jnp.broadcast_to(clip * graft, factor_ref.shape)
    pltpu.make_async_copy(sums.at[others], sums.at[others], sums_send).wait()


CHUNKS = 4


def scale(p_ref, factor_ref, out_hbm, scaled, sem):
    rows = p_ref.shape[0] // CHUNKS
    factor = factor_ref[0:1, 0:1]
    copies = []
    for i in range(CHUNKS):
        part = pl.ds(i * rows, rows)
        scaled[part, :] = (factor * p_ref[part, :]).astype(jnp.bfloat16)
        copies.append(pltpu.make_async_copy(scaled.at[part, :], out_hbm.at[part, :], sem.at[i]))
        copies[-1].start()
    for copy in copies:
        copy.wait()


def shards(nr, nc, grad, left_root, right_root):
    rows, width = grad.shape
    quarter = pltpu.VMEM((rows, width // 2), jnp.bfloat16)
    vmem = pl.BlockSpec(memory_space=pltpu.VMEM)
    grad, left_root, right_root = (
        pltpu.with_memory_space_constraint(a, pltpu.HBM) for a in (grad, left_root, right_root)
    )
    preconditioned, factor = pl.pallas_call(
        functools.partial(kernel, nr, nc),
        out_shape=(pltpu.VMEM((rows, width), F32), pltpu.VMEM((1, 128), F32)),
        in_specs=[pl.BlockSpec(memory_space=pltpu.HBM)] * 3,
        out_specs=(vmem, vmem),
        scratch_shapes=[quarter] * 11
        + [
            pltpu.VMEM((rows, width // 2), F32),
            pltpu.VMEM((nr * nc, 1, 128), F32),
            pltpu.VMEM((4, 1, 128), F32),
            pltpu.SemaphoreType.DMA((6,)),
            pltpu.SemaphoreType.DMA((4,)),
            pltpu.SemaphoreType.DMA((4,)),
            pltpu.SemaphoreType.DMA,
            pltpu.SemaphoreType.DMA,
            pltpu.SemaphoreType.REGULAR,
        ],
        compiler_params=pltpu.CompilerParams(
            collective_id=0, has_side_effects=True, vmem_limit_bytes=32 * 1024 * 1024
        ),
        name="shampoo",
    )(grad, left_root, right_root)
    return pl.pallas_call(
        scale,
        out_shape=jax.ShapeDtypeStruct((rows, width), jnp.bfloat16),
        in_specs=[vmem, vmem],
        out_specs=pl.BlockSpec(memory_space=pltpu.HBM),
        scratch_shapes=[pltpu.VMEM((rows, width), jnp.bfloat16), pltpu.SemaphoreType.DMA((CHUNKS,))],
        compiler_params=pltpu.CompilerParams(vmem_limit_bytes=16 * 1024 * 1024),
        name="scale",
    )(preconditioned, factor)


def solution(mesh):
    placed = (P(("row", "col"), None), P(("row", "col"), None), P(("row", "col"), None))
    return jax.shard_map(
        functools.partial(shards, mesh.shape["row"], mesh.shape["col"]),
        mesh=mesh, in_specs=placed, out_specs=P(("row", "col"), None), check_vma=False
    )
```

```python
import functools

import jax
import jax.numpy as jnp
from jax import lax
from jax.experimental import pallas as pl
from jax.experimental.pallas import tpu as pltpu
from jax.sharding import PartitionSpec as P

epsilon = 1e-06
clip_rms = 1.0
MESH = pl.DeviceIdType.MESH
F32 = jnp.float32


def nn(a, b):
    return jnp.dot(a, b, preferred_element_type=F32)


def nt(a, b):
    return lax.dot_general(a, b, (((1,), (1,)), ((), ())), preferred_element_type=F32)


def row_sq(x):
    s = jnp.sum(x * x, axis=0, keepdims=True)
    total = s[:, :128]
    for i in range(128, s.shape[1], 128):
        total = total + s[:, i : i + 128]
    return total


def group_size(nr, nc):
    return (2 if nr % 2 == 0 else 1) * nc


def kernel(nr, nc, g_hbm, l_hbm, r_hbm, p_ref, factor_ref,
           ga, gb, ra_own, ra_off, la, lb, rx, ra0, ra1, xa, xb, part,
           sums, pair, load_sem, send_sem, recv_sem, sums_send, sums_recv, ready):
    rows, width = g_hbm.shape
    devices = nr * nc
    members = group_size(nr, nc)
    row, col = lax.axis_index("row"), lax.axis_index("col")
    parity = lax.rem(col, 2)
    me = row * nc + col
    partner = (row, col + 1 - 2 * parity)

    def place(rank):
        return (lax.div(rank, nc), lax.rem(rank, nc))

    own = pl.ds(pl.multiple_of(parity * rows, rows), rows)
    off = pl.ds(pl.multiple_of((1 - parity) * rows, rows), rows)
    loads = []
    for i, (src, where, dst) in enumerate(
        ((g_hbm, own, ga), (g_hbm, off, gb), (r_hbm, own, ra_own), (r_hbm, off, ra_off),
         (l_hbm, own, la), (l_hbm, off, lb))
    ):
        loads.append(pltpu.make_async_copy(src.at[:, where], dst, load_sem.at[i]))
        if i < 4:
            loads[-1].start()

    barrier = pltpu.get_barrier_semaphore()

    def greet(rank, _):
        pl.semaphore_signal(barrier, inc=1, device_id=place(rank), device_id_type=MESH)

    lax.fori_loop(me - parity, me, greet, None)
    lax.fori_loop(me + 1, devices, greet, None)
    pl.semaphore_wait(barrier, me + 1 - parity)

    def say_ready(rank, _):
        pl.semaphore_signal(ready.at[lax.div(me, members)], inc=1, device_id=place(rank), device_id_type=MESH)

    lax.fori_loop(0, me, say_ready, None)

    sends = []

    def send(src, dst, device):
        i = len(sends)
        copy = pltpu.make_async_remote_copy(
            src_ref=src, dst_ref=dst, send_sem=send_sem.at[i], recv_sem=recv_sem.at[i],
            device_id=device, device_id_type=MESH)
        copy.start()
        sends.append(copy)
        return copy

    def send_sum(rank, _):
        pltpu.make_async_remote_copy(
            src_ref=pair.at[0], dst_ref=sums.at[me], send_sem=sums_send, recv_sem=sums_recv,
            device_id=place(rank), device_id_type=MESH).start()

    loads[0].wait()
    sq = row_sq(ga[...].astype(F32))
    loads[1].wait()
    sq = sq + row_sq(gb[...].astype(F32))
    pair[0] = sq
    loads[4].start()
    loads[5].start()
    head = jnp.minimum(me, 2)
    lax.fori_loop(0, head, send_sum, None)
    loads[2].wait()
    rx_copy = send(ra_own, rx, partner)
    loads[3].wait()
    ra0[...] = (nn(ga[...], ra_own[...]) + nt(gb[...], ra_off[...])).astype(jnp.bfloat16)
    xb_copy = send(ra0, xb, partner)
    lax.fori_loop(head, me, send_sum, None)

    part[...] = nn(ga[...], ra_off[...])
    loads[4].wait()
    p_ref[:, own] = nn(la[...], ra0[...])
    rx_copy.wait_recv()
    ra1[...] = (part[...] + nn(gb[...], rx[...])).astype(jnp.bfloat16)
    xa_copy = send(ra1, xa, partner)
    part[...] = nn(la[...], ra1[...])

    def send_up(group, _):
        first = jnp.maximum(me + 1, group * members)
        end = (group + 1) * members

        @pl.when(first < end)
        def _():
            pl.semaphore_wait(ready.at[group], end - first)
            lax.fori_loop(first, end, send_sum, None)

    lax.fori_loop(lax.div(me, members), devices // members, send_up, None)

    loads[5].wait()
    xb_copy.wait_recv()
    p1 = part[...] + nn(lb[...], xb[...])
    p_ref[:, off] = p1
    cond = row_sq(p1)
    xa_copy.wait_recv()
    p0 = p_ref[:, own] + nn(lb[...], xa[...])
    p_ref[:, own] = p0
    cond = cond + row_sq(p0)
    pair[1] = cond
    pair_copy = send(pair.at[pl.ds(0, 2)], pair.at[pl.ds(2, 2)], partner)


    count = width * width
    pair_copy.wait_recv()
    grad_sq = jnp.sum(sq + pair[2], axis=1, keepdims=True)
    cond_sq = jnp.sum(cond + pair[3], axis=1, keepdims=True)
    graft = jnp.sqrt((grad_sq / count + epsilon) / (cond_sq / count + epsilon))
    for copy in sends:
        copy.wait_send()

    sums[me] = sq
    others = pl.ds(0, devices - 1)
    pltpu.make_async_copy(sums.at[others], sums.at[others], sums_recv).wait()
    global_sq = jnp.sum(jnp.sum(sums[...], axis=0), axis=1, keepdims=True)
    clip = clip_rms / jnp.sqrt(global_sq / (devices * rows * width) + epsilon)
    factor_ref[...] = jnp.broadcast_to(clip * graft, factor_ref.shape)
    pltpu.make_async_copy(sums.at[others], sums.at[others], sums_send).wait()


CHUNKS = 4


def scale(p_ref, factor_ref, out_hbm, scaled, sem):
    rows = p_ref.shape[0] // CHUNKS
    factor = factor_ref[0:1, 0:1]
    copies = []
    for i in range(CHUNKS):
        part = pl.ds(i * rows, rows)
        scaled[part, :] = (factor * p_ref[part, :]).astype(jnp.bfloat16)
        copies.append(pltpu.make_async_copy(scaled.at[part, :], out_hbm.at[part, :], sem.at[i]))
        copies[-1].start()
    for copy in copies:
        copy.wait()


def shards(nr, nc, grad, left_root, right_root):
    rows, width = grad.shape
    quarter = pltpu.VMEM((rows, width // 2), jnp.bfloat16)
    vmem = pl.BlockSpec(memory_space=pltpu.VMEM)
    grad, left_root, right_root = (
        pltpu.with_memory_space_constraint(a, pltpu.HBM) for a in (grad, left_root, right_root)
    )
    preconditioned, factor = pl.pallas_call(
        functools.partial(kernel, nr, nc),
        out_shape=(pltpu.VMEM((rows, width), F32), pltpu.VMEM((1, 128), F32)),
        in_specs=[pl.BlockSpec(memory_space=pltpu.HBM)] * 3,
        out_specs=(vmem, vmem),
        scratch_shapes=[quarter] * 11
        + [
            pltpu.VMEM((rows, width // 2), F32),
            pltpu.VMEM((nr * nc, 1, 128), F32),
            pltpu.VMEM((4, 1, 128), F32),
            pltpu.SemaphoreType.DMA((6,)),
            pltpu.SemaphoreType.DMA((4,)),
            pltpu.SemaphoreType.DMA((4,)),
            pltpu.SemaphoreType.DMA,
            pltpu.SemaphoreType.DMA,
            pltpu.SemaphoreType.REGULAR((nr * nc // group_size(nr, nc),)),
        ],
        compiler_params=pltpu.CompilerParams(
            collective_id=0, has_side_effects=True, vmem_limit_bytes=32 * 1024 * 1024
        ),
        name="shampoo",
    )(grad, left_root, right_root)
    return pl.pallas_call(
        scale,
        out_shape=jax.ShapeDtypeStruct((rows, width), jnp.bfloat16),
        in_specs=[vmem, vmem],
        out_specs=pl.BlockSpec(memory_space=pltpu.HBM),
        scratch_shapes=[pltpu.VMEM((rows, width), jnp.bfloat16), pltpu.SemaphoreType.DMA((CHUNKS,))],
        compiler_params=pltpu.CompilerParams(vmem_limit_bytes=16 * 1024 * 1024),
        name="scale",
    )(preconditioned, factor)


def solution(mesh):
    placed = (P(("row", "col"), None), P(("row", "col"), None), P(("row", "col"), None))
    return jax.shard_map(
        functools.partial(shards, mesh.shape["row"], mesh.shape["col"]),
        mesh=mesh, in_specs=placed, out_specs=P(("row", "col"), None), check_vma=False
    )
```
